32 devices in a mesh: rep: 2 (over z, core), dp: 16 (over x, y).
Axes of the slice: x: 4, y: 4, z: 1, core: 2. Of those that a mesh axis runs over, the one named last changes fastest.
The devices are a block of a 4x4x8 slice.
Arguments:
- x: bfloat16 [32, 2048, 512], P(('rep', 'dp')), parts along dimension 0
- dy: bfloat16 [32, 2048, 512], P(('rep', 'dp')), parts along dimension 0
- w_gate: bfloat16 [2, 512, 3072], replicated
- w_up: bfloat16 [2, 512, 3072], replicated
- w_down: bfloat16 [2, 3072, 512], replicated
- m_w_gate: float32 [2, 512, 3072], replicated
- m_w_up: float32 [2, 512, 3072], replicated
- m_w_down: float32 [2, 3072, 512], replicated
- v_w_gate: float32 [2, 512, 3072], replicated
- v_w_up: float32 [2, 512, 3072], replicated
- v_w_down: float32 [2, 3072, 512], replicated
Outputs:
- output 1: bfloat16 [4, 512, 3072], P('rep'), parts along dimension 0
- output 2: bfloat16 [4, 512, 3072], P('rep'), parts along dimension 0
- output 3: bfloat16 [4, 3072, 512], P('rep'), parts along dimension 0
- output 4: float32 [4, 512, 3072], P('rep'), parts along dimension 0
- output 5: float32 [4, 512, 3072], P('rep'), parts along dimension 0
- output 6: float32 [4, 3072, 512], P('rep'), parts along dimension 0
- output 7: float32 [4, 512, 3072], P('rep'), parts along dimension 0
- output 8: float32 [4, 512, 3072], P('rep'), parts along dimension 0
- output 9: float32 [4, 3072, 512], P('rep'), parts along dimension 0
There are 2 independent parts. The reference program is written for one: setup_inputs(seed, part) draws one part's arguments, and reference() takes and returns one part's arrays. A program takes and returns all parts, laid end to end along the dimension named above; an argument that names none is the same for every part.
All inputs are finite; a program needn't handle non-finite values.
Results may differ from the reference program's by a relative error of at most 0.022.
Values are sent between devices in bfloat16 or wider.
A program may use at most 768 MiB of HBM per device.

```python
import jax
import jax.numpy as jnp
from jax import lax

SEQUENCES = 16
TOKENS = 2048
D = 512
FF = 3072
LAYERS = 2
NAMES = ("w_gate", "w_up", "w_down")
SHAPES = {"w_gate": (LAYERS, D, FF), "w_up": (LAYERS, D, FF), "w_down": (LAYERS, FF, D)}


def bump(key, n, height):
    away = (jnp.arange(n, dtype=jnp.int32) - jax.random.randint(key, (), 0, n, jnp.int32)) % n
    return jnp.where(away < n // 8, height, 1.0)


def together(key, own, strength):
    shared = jax.random.normal(key, own.shape[1:], jnp.float32)
    return (own + strength * shared) * lax.rsqrt(1 + strength * strength)


def setup_inputs(seed: int = 0, part: int = 0) -> dict:
    kx, kdy, ka, kb, kz, kf, kh, kl, *keys = jax.random.split(jax.random.key(seed), 8 + 3 * len(NAMES))
    kx, kdy, ka, kb = (jax.random.fold_in(k, part) for k in (kx, kdy, ka, kb))
    kw, km, kv = (keys[i::3] for i in range(3))
    shape = (SEQUENCES, TOKENS, D)
    much_x, much_dy = jax.random.uniform(kz, (2,), jnp.float32, 0.0, 1.0)
    loud = 2.0 ** jax.random.uniform(jax.random.fold_in(kz, 1), (), jnp.float32, -1.0, 2.0)
    layers = 2.0 ** jax.random.uniform(kl, (LAYERS, 1, 1), jnp.float32, -1.0, 1.0)
    x = together(ka, jax.random.normal(kx, shape, jnp.float32), much_x) * bump(kf, D, 4.0)
    dy = together(kb, jax.random.normal(kdy, shape, jnp.float32), much_dy)
    drawn = {"x": x.astype(jnp.bfloat16), "dy": (loud * dy * (SEQUENCES * TOKENS) ** -0.5).astype(jnp.bfloat16)}
    for key, name in zip(kw, NAMES, strict=True):
        w = jax.random.normal(key, SHAPES[name], jnp.float32) * SHAPES[name][1] ** -0.5
        drawn[name] = (w * {"w_gate": 1.0, "w_up": bump(kh, FF, 4.0), "w_down": layers}[name]).astype(jnp.bfloat16)
    for key, name in zip(km, NAMES, strict=True):
        drawn[f"m_{name}"] = 0.1 * jax.random.normal(key, SHAPES[name], jnp.float32)
    for key, name in zip(kv, NAMES, strict=True):
        drawn[f"v_{name}"] = jax.random.uniform(key, SHAPES[name], jnp.float32, 0.005, 0.015)
    return drawn


def matmul(a, w):
    return jnp.dot(a, w, preferred_element_type=jnp.float32).astype(jnp.bfloat16)


def normed(h):
    wide = h.astype(jnp.float32)
    scale = lax.rsqrt(jnp.mean(wide**2, -1, keepdims=True) + 1e-6)
    return (wide * scale).astype(jnp.bfloat16)


def layer(h, w):
    a = normed(h)
    gate = jnp.dot(a, w["w_gate"], preferred_element_type=jnp.float32)
    up = jnp.dot(a, w["w_up"], preferred_element_type=jnp.float32)
    return h + matmul((jax.nn.silu(gate) * up).astype(jnp.bfloat16), w["w_down"])


def adamw(w, m, v, g):
    m = 0.9 * m + 0.1 * g
    v = 0.95 * v + 0.05 * g * g
    step = m * lax.rsqrt(v + 1e-8) + 0.1 * w
    return (w - 0.02 * step).astype(jnp.bfloat16), m, v


def stack(weights, h):
    return lax.scan(lambda h, w: (layer(h, w), None), h, weights)[0]


def reference(x, dy, w_gate, w_up, w_down, m_w_gate, m_w_up, m_w_down, v_w_gate, v_w_up, v_w_down):
    weights = dict(zip(NAMES, (w_gate, w_up, w_down), strict=True))

    def take(so_far, sequence):
        h, by_y = sequence
        _, back = jax.vjp(lambda w: stack(w, h), weights)
        return jax.tree.map(lambda total, term: total + term.astype(jnp.float32), so_far, back(by_y)[0]), None

    none_yet = {name: jnp.zeros(w.shape, jnp.float32) for name, w in weights.items()}
    by_weights, _ = lax.scan(take, none_yet, (x, dy))
    gradients = [by_weights[name].astype(jnp.bfloat16).astype(jnp.float32) for name in NAMES]
    new = [
        adamw(w.astype(jnp.float32), m, v, g)
        for w, m, v, g in zip((w_gate, w_up, w_down), (m_w_gate, m_w_up, m_w_down), (v_w_gate, v_w_up, v_w_down), gradients, strict=True)
    ]
    return tuple(one[which] for which in range(3) for one in new)
```

```python
import functools
import math

import jax
import jax.numpy as jnp
from jax import lax
from jax.experimental import pallas as pl
from jax.experimental.pallas import tpu as pltpu
from jax.sharding import PartitionSpec as P

BLOCK = 512
TILE = 512
SLOTS = 4
STAGES = 8
VMEM_LIMIT = 67_043_328
F32, BF16 = jnp.float32, jnp.bfloat16
NN = (((1,), (0,)), ((), ()))
NT = (((1,), (1,)), ((), ()))


def dot(a, b, dims=NN):
    return lax.dot_general(a, b, dims, preferred_element_type=F32)


def scale_of(wide):
    return lax.rsqrt(jnp.mean(wide * wide, -1, keepdims=True) + 1e-6)


def normed(h):
    wide = h.astype(F32)
    return (wide * scale_of(wide)).astype(BF16)


def train_kernel(
    side, x_hbm, dy_hbm, wg_hbm, wu_hbm, wd_hbm, out_hbm,
    x, a, at, dh, dht, act, dg, du, acc1, acc2, wg, wu, wd,
    grad, r1, r2, part, t1, u1, t2, u2, own, send, recv, w_sem, x_sem, own_sem,
):
    tokens, d = x.shape
    blocks = wg_hbm.shape[2] // BLOCK
    chunks = wg_hbm.shape[0] * blocks
    tiles = tokens // TILE
    half_rows = grad.shape[2] // 2
    n1, n2 = half_rows // side, half_rows // side // side
    cols = BLOCK // 2

    me = lax.axis_index("dp")
    ix, iy = me // side, lax.rem(me, side)

    def turn(i, by):
        return lax.rem(i + (by + side), side)

    along_x = (ix, tuple(turn(ix, s) * side + iy for s in (1, -1)))
    along_y = (iy, tuple(ix * side + turn(iy, s) for s in (1, -1)))
    flows = ((along_x, along_y), (along_y, along_x))
    step_of = (1, -1)

    barrier = pltpu.get_barrier_semaphore()
    for _, near in (along_x, along_y):
        for device in near:
            pl.semaphore_signal(barrier, inc=1, device_id={"dp": device}, device_id_type=pl.DeviceIdType.MESH)

    def rows(flow, s1, s2=None):
        if s2 is None:
            return pl.ds(pl.multiple_of(flow * half_rows + s1 * n1, 16), n1)
        return pl.ds(pl.multiple_of(flow * half_rows + s1 * n1 + s2 * n2, 16), n2)

    def hop(stage, c, flow, way):
        slot = lax.rem(c, SLOTS)
        (i1, near1), (i2, near2) = flows[flow]
        step = step_of[way]
        if stage == 0:
            src, dst, to = grad.at[slot, way, rows(flow, turn(i1, 2)), :], r1.at[slot, flow, way], near1
        elif stage == 1:
            src, dst, to = grad.at[slot, :, rows(flow, turn(i1, step)), :], r2.at[slot, flow, way], near1
        elif stage == 2:
            src, dst, to = t1.at[slot, flow, way], u1.at[slot, flow, way], near2
        elif stage == 3:
            src, dst, to = t2.at[slot, flow, way], u2.at[slot, flow, way], near2
        elif stage == 4:
            src, dst, to = own.at[slot, flow], out_hbm.at[c, :, rows(flow, i1, i2), :], near2
        elif stage == 5:
            src = dst = out_hbm.at[c, way, rows(flow, i1, turn(i2, -step)), :]
            to = near2
        elif stage == 6:
            src = dst = out_hbm.at[c, :, rows(flow, i1), :]
            to = near1
        else:
            src = dst = out_hbm.at[c, way, rows(flow, turn(i1, -step)), :]
            to = near1
        return pltpu.make_async_remote_copy(
            src_ref=src,
            dst_ref=dst,
            send_sem=send.at[slot, stage, flow, way],
            recv_sem=recv.at[slot, stage, flow, way],
            device_id={"dp": to[way]},
            device_id_type=pl.DeviceIdType.MESH,
        )

    def keep(c, flow):
        slot = lax.rem(c, SLOTS)
        (i1, _), (i2, _) = flows[flow]
        return pltpu.make_async_copy(own.at[slot, flow], out_hbm.at[c, :, rows(flow, i1, i2), :], own_sem.at[slot, flow])

    def wait(stage, c):
        for flow in range(2):
            for way in range(2):
                hop(stage, c, flow, way).wait()

    def start(stage, c):
        for flow in range(2):
            for way in range(2):
                hop(stage, c, flow, way).start()

    def advance(event, c):
        slot, pslot = lax.rem(c, SLOTS), lax.rem(c, 2)
        wait(event - 1, c)
        for flow in range(2):
            (i1, _), (i2, _) = flows[flow]
            if event == 1:
                for way in range(2):
                    where = rows(flow, turn(i1, step_of[way]))
                    total = grad[slot, way, where, :].astype(F32) + r1[slot, flow, way].astype(F32)
                    grad[slot, way, where, :] = total.astype(BF16)
            elif event == 2:
                for h in range(2):
                    mine = grad[slot, h, rows(flow, i1), :].astype(F32)
                    part[pslot, flow, h] = mine + r2[slot, flow, 0, h].astype(F32) + r2[slot, flow, 1, h].astype(F32)
                far = pl.ds(pl.multiple_of(turn(i2, 2) * n2, 16), n2)
                for way in range(2):
                    t1[slot, flow, way] = part[pslot, flow, way, far, :].astype(BF16)
            elif event == 3:
                for way in range(2):
                    near = pl.ds(pl.multiple_of(turn(i2, step_of[way]) * n2, 16), n2)
                    for h in range(2):
                        total = part[pslot, flow, h, near, :]
                        if h == way:
                            total = total + u1[slot, flow, way].astype(F32)
                        t2[slot, flow, way, h] = total.astype(BF16)
            elif event == 4:
                here = pl.ds(pl.multiple_of(i2 * n2, 16), n2)
                for h in range(2):
                    total = part[pslot, flow, h, here, :] + u2[slot, flow, 0, h].astype(F32) + u2[slot, flow, 1, h].astype(F32)
                    own[slot, flow, h] = total.astype(BF16)
                keep(c, flow).start()
            elif event == 5:
                keep(c, flow).wait()
        if event < STAGES:
            start(event, c)

    def poll(k, events):
        for behind, event in events:
            c = k - behind

            @pl.when((c >= 0) & (c < chunks))
            def _(c=c, event=event):
                advance(event, c)

    def poll_mid(k):
        poll(k, ((4, 7), (3, 5), (2, 3), (1, 1)))

    def poll_end(k):
        poll(k, ((4, 8), (3, 6), (2, 4), (1, 2)))

    def weights(b):
        layer, j, slot = lax.rem(b // blocks, 2), lax.rem(b, blocks), lax.rem(b, 2)
        span = pl.ds(pl.multiple_of(j * BLOCK, BLOCK), BLOCK)
        return (
            pltpu.make_async_copy(wg_hbm.at[layer, :, span], wg.at[slot], w_sem.at[slot, 0]),
            pltpu.make_async_copy(wu_hbm.at[layer, :, span], wu.at[slot], w_sem.at[slot, 1]),
            pltpu.make_async_copy(wd_hbm.at[layer, span, :], wd.at[slot], w_sem.at[slot, 2]),
        )

    def next_weights(b):
        for copy in weights(b):
            copy.wait()

        @pl.when(b + 1 < 3 * blocks)
        def _():
            for copy in weights(b + 1):
                copy.start()

    def each_tile(body):
        @pl.loop(0, tiles)
        def _(t):
            body(pl.ds(pl.multiple_of(t * TILE, TILE), TILE))

    load_x = pltpu.make_async_copy(x_hbm.at[0], x, x_sem.at[0])
    load_dy = pltpu.make_async_copy(dy_hbm.at[0], dh, x_sem.at[1])
    load_x.start()
    for copy in weights(0):
        copy.start()
    load_dy.start()
    load_x.wait()

    def first(t):
        a[t, :] = normed(x[t, :])
        acc1[t, :] = jnp.zeros((TILE, d), F32)

    each_tile(first)

    @pl.loop(0, blocks)
    def _(b):
        next_weights(b)
        slot = lax.rem(b, 2)

        def forward(t):
            gate = dot(a[t, :], wg[slot])
            up = dot(a[t, :], wu[slot])
            acc1[t, :] += dot((jax.nn.silu(gate) * up).astype(BF16), wd[slot])

        each_tile(forward)

    load_dy.wait()

    def second(t):
        h = (x[t, :].astype(F32) + acc1[t, :].astype(BF16).astype(F32)).astype(BF16)
        x[t, :] = h
        after = normed(h)
        a[t, :] = after
        at[:, t] = after.T
        dht[:, t] = dh[t, :].T
        acc1[t, :] = jnp.zeros((TILE, d), F32)
        acc2[t, :] = jnp.zeros((TILE, d), F32)

    each_tile(second)
    pl.semaphore_wait(barrier, 4)

    def backward(k, to_input):
        next_weights(k + blocks)
        slot, gslot = lax.rem(k + blocks, 2), lax.rem(k, SLOTS)

        def states(t):
            gate = dot(a[t, :], wg[slot])
            up = dot(a[t, :], wu[slot])
            by_act = dot(dh[t, :], wd[slot], NT).astype(BF16).astype(F32)
            s = jax.nn.sigmoid(gate)
            silu = gate * s
            act[t, :] = (silu * up).astype(BF16)
            by_up = (by_act * silu).astype(BF16)
            by_gate = (by_act * up * (s * (1.0 + gate * (1.0 - s)))).astype(BF16)
            dg[t, :] = by_gate
            du[t, :] = by_up
            if to_input:
                acc1[t, :] += dot(by_gate, wg[slot], NT)
                acc2[t, :] += dot(by_up, wu[slot], NT)

        each_tile(states)
        poll_mid(k)
        for h in range(2):
            span = slice(h * cols, (h + 1) * cols)
            grad[gslot, h, 0:d, :] = dot(at[...], dg[:, span]).astype(BF16)
            grad[gslot, h, d : 2 * d, :] = dot(at[...], du[:, span]).astype(BF16)
            grad[gslot, h, 2 * d : 3 * d, :] = dot(dht[...], act[:, span]).astype(BF16)
        start(0, k)
        poll_end(k)

    @pl.loop(0, blocks)
    def _(k):
        backward(k, True)

    again = pltpu.make_async_copy(x_hbm.at[0], act, x_sem.at[0])
    again.start()

    def between(t):
        by_a = (acc1[t, :].astype(BF16).astype(F32) + acc2[t, :].astype(BF16).astype(F32)).astype(BF16).astype(F32)
        wide = x[t, :].astype(F32)
        scale = scale_of(wide)
        along = jnp.sum(by_a * wide, -1, keepdims=True) * (scale * scale * scale / d)
        by_h = (by_a * scale - wide * along).astype(BF16)
        total = (dh[t, :].astype(F32) + by_h.astype(F32)).astype(BF16)
        dh[t, :] = total
        dht[:, t] = total.T

    each_tile(between)
    again.wait()

    def first_again(t):
        before = normed(act[t, :])
        a[t, :] = before
        at[:, t] = before.T

    each_tile(first_again)

    @pl.loop(blocks, 2 * blocks)
    def _(k):
        backward(k, False)

    @pl.loop(2 * blocks, 2 * blocks + 4)
    def _(k):
        poll_mid(k)
        poll_end(k)


def gradients(side, x, dy, wg, wu, wd):
    _, tokens, d = x.shape
    layers, _, ff = wg.shape
    chunks, high, cols = layers * ff // BLOCK, 3 * d, BLOCK // 2
    n1, n2 = high // 2 // side, high // 2 // side // side
    flops = 2 * tokens * d * ff * 17
    vmem = pltpu.VMEM
    return pl.pallas_call(
        functools.partial(train_kernel, side),
        out_shape=jax.ShapeDtypeStruct((chunks, 2, high, cols), BF16),
        in_specs=[pl.BlockSpec(memory_space=pl.ANY)] * 5,
        out_specs=pl.BlockSpec(memory_space=pl.ANY),
        scratch_shapes=[
            vmem((tokens, d), BF16),
            vmem((tokens, d), BF16),
            vmem((d, tokens), BF16),
            vmem((tokens, d), BF16),
            vmem((d, tokens), BF16),
            vmem((tokens, BLOCK), BF16),
            vmem((tokens, BLOCK), BF16),
            vmem((tokens, BLOCK), BF16),
            vmem((tokens, d), F32),
            vmem((tokens, d), F32),
            vmem((2, d, BLOCK), BF16),
            vmem((2, d, BLOCK), BF16),
            vmem((2, BLOCK, d), BF16),
            vmem((SLOTS, 2, high, cols), BF16),
            vmem((SLOTS, 2, 2, n1, cols), BF16),
            vmem((SLOTS, 2, 2, 2, n1, cols), BF16),
            vmem((2, 2, 2, n1, cols), F32),
            vmem((SLOTS, 2, 2, n2, cols), BF16),
            vmem((SLOTS, 2, 2, n2, cols), BF16),
            vmem((SLOTS, 2, 2, 2, n2, cols), BF16),
            vmem((SLOTS, 2, 2, 2, n2, cols), BF16),
            vmem((SLOTS, 2, 2, n2, cols), BF16),
            pltpu.SemaphoreType.DMA((SLOTS, STAGES, 2, 2)),
            pltpu.SemaphoreType.DMA((SLOTS, STAGES, 2, 2)),
            pltpu.SemaphoreType.DMA((2, 3)),
            pltpu.SemaphoreType.DMA((2,)),
            pltpu.SemaphoreType.DMA((SLOTS, 2)),
        ],
        compiler_params=pltpu.CompilerParams(collective_id=0, has_side_effects=True, vmem_limit_bytes=VMEM_LIMIT),
        cost_estimate=pl.CostEstimate(flops=flops, bytes_accessed=4 * wg.size * 3, transcendentals=tokens * ff * 6),
        name="train",
    )(x, dy, wg, wu, wd)


def adamw_kernel(d, g_ref, *refs):
    ins, outs = refs[:9], refs[9:]
    for i in range(3):
        g = g_ref[0, 0, i * d : (i + 1) * d, :]
        g = (g.T if i == 2 else g).astype(F32)
        m = 0.9 * ins[3 + i][0] + 0.1 * g
        v = 0.95 * ins[6 + i][0] + 0.05 * g * g
        w = ins[i][0].astype(F32)
        step = m * lax.rsqrt(v + 1e-8) + 0.1 * w
        outs[i][0] = (w - 0.02 * step).astype(BF16)
        outs[3 + i][0] = m
        outs[6 + i][0] = v


def adamw(g, arrays):
    layers, d, ff = arrays[0].shape
    blocks = ff // BLOCK
    cols = BLOCK // 2

    def across(c, h):
        return layers - 1 - c // blocks, 0, lax.rem(c, blocks) * 2 + h

    def down(c, h):
        return layers - 1 - c // blocks, lax.rem(c, blocks) * 2 + h, 0

    specs = [pl.BlockSpec((1, d, cols), across), pl.BlockSpec((1, d, cols), across), pl.BlockSpec((1, cols, d), down)] * 3
    return pl.pallas_call(
        functools.partial(adamw_kernel, d),
        grid=(g.shape[0], 2),
        out_shape=[jax.ShapeDtypeStruct(one.shape, one.dtype) for one in arrays],
        in_specs=[pl.BlockSpec((1, 1, 3 * d, cols), lambda c, h: (c, h, 0, 0)), *specs],
        out_specs=specs,
        compiler_params=pltpu.CompilerParams(vmem_limit_bytes=60_000_000),
        cost_estimate=pl.CostEstimate(flops=20 * g.size, bytes_accessed=22 * g.size, transcendentals=g.size),
        name="adamw",
    )(g, *arrays)


def solution(mesh):
    side = math.isqrt(mesh.shape["dp"])
    assert side == 4 and side * side == mesh.shape["dp"]

    def step(x, dy, *arrays):
        g = gradients(side, x, dy, *arrays[:3])
        return tuple(adamw(g, arrays))

    return jax.shard_map(
        step,
        mesh=mesh,
        in_specs=(P(("rep", "dp"), None, None),) * 2 + (P(None, None, None),) * 9,
        out_specs=(P("rep", None, None),) * 9,
        check_vma=False,
    )
```

```python
import functools
import math

import jax
import jax.numpy as jnp
from jax import lax
from jax.experimental import pallas as pl
from jax.experimental.pallas import tpu as pltpu
from jax.sharding import PartitionSpec as P

BLOCK = 512
TILE = 1024
LATE = 4
SLOTS = 4
STAGES = 8
VMEM_LIMIT = 67_043_328
F32, BF16 = jnp.float32, jnp.bfloat16
NN = (((1,), (0,)), ((), ()))
NT = (((1,), (1,)), ((), ()))


def dot(a, b, dims=NN):
    return lax.dot_general(a, b, dims, preferred_element_type=F32)


def scale_of(wide):
    return lax.rsqrt(jnp.mean(wide * wide, -1, keepdims=True) + 1e-6)


def normed(h):
    wide = h.astype(F32)
    return (wide * scale_of(wide)).astype(BF16)


def train_kernel(
    side, x_hbm, dy_hbm, wg_hbm, wu_hbm, wd_hbm, out_hbm, late0, late1,
    x, a, at, dh, dht, act, dg, du, acc1, acc2, wg, wu, wd,
    grad, r1, r2, part, t1, u1, t2, u2, own, send, recv, w_sem, x_sem, own_sem,
):
    tokens, d = x.shape
    blocks = wg_hbm.shape[2] // BLOCK
    chunks = wg_hbm.shape[0] * blocks
    tiles = tokens // TILE
    cut = out_hbm.shape[0]
    lates = (late0, late1)
    half_rows = grad.shape[2] // 2
    n1, n2 = half_rows // side, half_rows // side // side
    cols = BLOCK // 2

    me = lax.axis_index("dp")
    ix, iy = me // side, lax.rem(me, side)

    def turn(i, by):
        return lax.rem(i + (by + side), side)

    along_x = (ix, tuple(turn(ix, s) * side + iy for s in (1, -1)))
    along_y = (iy, tuple(ix * side + turn(iy, s) for s in (1, -1)))
    flows = ((along_x, along_y), (along_y, along_x))
    step_of = (1, -1)

    barrier = pltpu.get_barrier_semaphore()
    for _, near in (along_x, along_y):
        for device in near:
            pl.semaphore_signal(barrier, inc=1, device_id={"dp": device}, device_id_type=pl.DeviceIdType.MESH)

    def rows(flow, s1, s2=None):
        if s2 is None:
            return pl.ds(pl.multiple_of(flow * half_rows + s1 * n1, 16), n1)
        return pl.ds(pl.multiple_of(flow * half_rows + s1 * n1 + s2 * n2, 16), n2)

    def gathered(c, flow, i1, i2, late, way=slice(None)):
        if late:
            return lates[flow].at[way, c - cut, pl.ds(pl.multiple_of(i2 * n2, 16), n2), :]
        return out_hbm.at[c, way, rows(flow, i1, i2), :]

    def hop(stage, c, flow, way, late):
        slot = lax.rem(c, SLOTS)
        (i1, near1), (i2, near2) = flows[flow]
        step = step_of[way]
        if stage == 0:
            src, dst, to = grad.at[slot, way, rows(flow, turn(i1, 2)), :], r1.at[slot, flow, way], near1
        elif stage == 1:
            src, dst, to = grad.at[slot, :, rows(flow, turn(i1, step)), :], r2.at[slot, flow, way], near1
        elif stage == 2:
            src, dst, to = t1.at[slot, flow, way], u1.at[slot, flow, way], near2
        elif stage == 3:
            src, dst, to = t2.at[slot, flow, way], u2.at[slot, flow, way], near2
        elif stage == 4:
            src, dst, to = own.at[slot, flow], gathered(c, flow, i1, i2, late), near2
        elif stage == 5:
            src = dst = gathered(c, flow, i1, turn(i2, -step), late, way)
            to = near2
        elif stage == 6:
            src = dst = out_hbm.at[c, :, rows(flow, i1), :]
            to = near1
        else:
            src = dst = out_hbm.at[c, way, rows(flow, turn(i1, -step)), :]
            to = near1
        return pltpu.make_async_remote_copy(
            src_ref=src,
            dst_ref=dst,
            send_sem=send.at[slot, stage, flow, way],
            recv_sem=recv.at[slot, stage, flow, way],
            device_id={"dp": to[way]},
            device_id_type=pl.DeviceIdType.MESH,
        )

    def keep(c, flow, late):
        slot = lax.rem(c, SLOTS)
        (i1, _), (i2, _) = flows[flow]
        return pltpu.make_async_copy(own.at[slot, flow], gathered(c, flow, i1, i2, late), own_sem.at[slot, flow])

    def wait(stage, c, late=False):
        for flow in range(2):
            for way in range(2):
                hop(stage, c, flow, way, late).wait()

    def start(stage, c, late=False):
        for flow in range(2):
            for way in range(2):
                hop(stage, c, flow, way, late).start()

    def advance(event, c, late):
        slot, pslot = lax.rem(c, SLOTS), lax.rem(c, 2)
        wait(event - 1, c, late)
        for flow in range(2):
            (i1, _), (i2, _) = flows[flow]
            if event == 1:
                for way in range(2):
                    where = rows(flow, turn(i1, step_of[way]))
                    total = grad[slot, way, where, :].astype(F32) + r1[slot, flow, way].astype(F32)
                    grad[slot, way, where, :] = total.astype(BF16)
            elif event == 2:
                for h in range(2):
                    mine = grad[slot, h, rows(flow, i1), :].astype(F32)
                    part[pslot, flow, h] = mine + r2[slot, flow, 0, h].astype(F32) + r2[slot, flow, 1, h].astype(F32)
                far = pl.ds(pl.multiple_of(turn(i2, 2) * n2, 16), n2)
                for way in range(2):
                    t1[slot, flow, way] = part[pslot, flow, way, far, :].astype(BF16)
            elif event == 3:
                for way in range(2):
                    near = pl.ds(pl.multiple_of(turn(i2, step_of[way]) * n2, 16), n2)
                    for h in range(2):
                        total = part[pslot, flow, h, near, :]
                        if h == way:
                            total = total + u1[slot, flow, way].astype(F32)
                        t2[slot, flow, way, h] = total.astype(BF16)
            elif event == 4:
                here = pl.ds(pl.multiple_of(i2 * n2, 16), n2)
                for h in range(2):
                    total = part[pslot, flow, h, here, :] + u2[slot, flow, 0, h].astype(F32) + u2[slot, flow, 1, h].astype(F32)
                    own[slot, flow, h] = total.astype(BF16)
                keep(c, flow, late).start()
            elif event == 5:
                keep(c, flow, late).wait()
        if event < (6 if late else STAGES):
            start(event, c, late)

    def poll(k, events):
        for behind, event in events:
            c = k - behind

            @pl.when((c >= 0) & (c < (cut if event > 3 else chunks)))
            def _(c=c, event=event):
                advance(event, c, False)

            if 3 < event < 7:

                @pl.when((c >= cut) & (c < chunks))
                def _(c=c, event=event):
                    advance(event, c, True)

    def poll_mid(k):
        poll(k, ((4, 7), (3, 5), (1, 1), (2, 3)))

    def poll_end(k):
        poll(k, ((4, 8), (3, 6), (2, 4), (1, 2)))

    def weights(b):
        layer, j, slot = lax.rem(b // blocks, 2), lax.rem(b, blocks), lax.rem(b, 2)
        span = pl.ds(pl.multiple_of(j * BLOCK, BLOCK), BLOCK)
        return (
            pltpu.make_async_copy(wg_hbm.at[layer, :, span], wg.at[slot], w_sem.at[slot, 0]),
            pltpu.make_async_copy(wu_hbm.at[layer, :, span], wu.at[slot], w_sem.at[slot, 1]),
            pltpu.make_async_copy(wd_hbm.at[layer, span, :], wd.at[slot], w_sem.at[slot, 2]),
        )

    def next_weights(b):
        for copy in weights(b):
            copy.wait()

        @pl.when(b + 1 < 3 * blocks)
        def _():
            for copy in weights(b + 1):
                copy.start()

    def each_tile(body):
        @pl.loop(0, tiles)
        def _(t):
            body(pl.ds(pl.multiple_of(t * TILE, TILE), TILE))

    load_x = pltpu.make_async_copy(x_hbm.at[0], x, x_sem.at[0])
    load_dy = pltpu.make_async_copy(dy_hbm.at[0], dh, x_sem.at[1])
    load_x.start()
    for copy in weights(0):
        copy.start()
    load_dy.start()
    load_x.wait()

    def first(t):
        a[t, :] = normed(x[t, :])
        acc1[t, :] = jnp.zeros((TILE, d), F32)

    each_tile(first)

    @pl.loop(0, blocks)
    def _(b):
        next_weights(b)
        slot = lax.rem(b, 2)

        def forward(t):
            gate = dot(a[t, :], wg[slot])
            up = dot(a[t, :], wu[slot])
            acc1[t, :] += dot((jax.nn.silu(gate) * up).astype(BF16), wd[slot])

        each_tile(forward)

    load_dy.wait()

    def second(t):
        h = (x[t, :].astype(F32) + acc1[t, :].astype(BF16).astype(F32)).astype(BF16)
        x[t, :] = h
        after = normed(h)
        a[t, :] = after
        at[:, t] = after.T
        dht[:, t] = dh[t, :].T
        acc1[t, :] = jnp.zeros((TILE, d), F32)
        acc2[t, :] = jnp.zeros((TILE, d), F32)

    each_tile(second)
    pl.semaphore_wait(barrier, 4)

    def backward(k, to_input):
        next_weights(k + blocks)
        slot, gslot = lax.rem(k + blocks, 2), lax.rem(k, SLOTS)

        def states(t):
            gate = dot(a[t, :], wg[slot])
            up = dot(a[t, :], wu[slot])
            by_act = dot(dh[t, :], wd[slot], NT).astype(BF16).astype(F32)
            s = jax.nn.sigmoid(gate)
            silu = gate * s
            act[t, :] = (silu * up).astype(BF16)
            by_up = (by_act * silu).astype(BF16)
            by_gate = (by_act * up * (s * (1.0 + gate * (1.0 - s)))).astype(BF16)
            dg[t, :] = by_gate
            du[t, :] = by_up
            if to_input:
                acc1[t, :] += dot(by_gate, wg[slot], NT)
                acc2[t, :] += dot(by_up, wu[slot], NT)

        each_tile(states)
        poll_mid(k)
        for h in range(2):
            span = slice(h * cols, (h + 1) * cols)
            grad[gslot, h, 0:d, :] = dot(at[...], dg[:, span]).astype(BF16)
            grad[gslot, h, d : 2 * d, :] = dot(at[...], du[:, span]).astype(BF16)
            grad[gslot, h, 2 * d : 3 * d, :] = dot(dht[...], act[:, span]).astype(BF16)
        start(0, k)
        poll_end(k)

    @pl.loop(0, blocks)
    def _(k):
        backward(k, True)

    def between(t):
        by_a = (acc1[t, :].astype(BF16).astype(F32) + acc2[t, :].astype(BF16).astype(F32)).astype(BF16).astype(F32)
        wide = x[t, :].astype(F32)
        scale = scale_of(wide)
        along = jnp.sum(by_a * wide, -1, keepdims=True) * (scale * scale * scale / d)
        by_h = (by_a * scale - wide * along).astype(BF16)
        total = (dh[t, :].astype(F32) + by_h.astype(F32)).astype(BF16)
        dh[t, :] = total
        dht[:, t] = total.T

    each_tile(between)
    load_x.start()
    load_x.wait()

    def first_again(t):
        before = normed(x[t, :])
        a[t, :] = before
        at[:, t] = before.T

    each_tile(first_again)

    @pl.loop(blocks, 2 * blocks)
    def _(k):
        backward(k, False)

    @pl.loop(2 * blocks, 2 * blocks + 3)
    def _(k):
        poll_mid(k)
        poll_end(k)


def gradients(side, x, dy, wg, wu, wd):
    _, tokens, d = x.shape
    layers, _, ff = wg.shape
    chunks, high, cols = layers * ff // BLOCK, 3 * d, BLOCK // 2
    n1, n2 = high // 2 // side, high // 2 // side // side
    flops = 2 * tokens * d * ff * 17
    vmem = pltpu.VMEM
    return pl.pallas_call(
        functools.partial(train_kernel, side),
        out_shape=[
            jax.ShapeDtypeStruct((chunks - LATE, 2, high, cols), BF16),
            jax.ShapeDtypeStruct((2, LATE, n1, cols), BF16),
            jax.ShapeDtypeStruct((2, LATE, n1, cols), BF16),
        ],
        in_specs=[pl.BlockSpec(memory_space=pl.ANY)] * 5,
        out_specs=[pl.BlockSpec(memory_space=pl.ANY)] * 3,
        scratch_shapes=[
            vmem((tokens, d), BF16),
            vmem((tokens, d), BF16),
            vmem((d, tokens), BF16),
            vmem((tokens, d), BF16),
            vmem((d, tokens), BF16),
            vmem((tokens, BLOCK), BF16),
            vmem((tokens, BLOCK), BF16),
            vmem((tokens, BLOCK), BF16),
            vmem((tokens, d), F32),
            vmem((tokens, d), F32),
            vmem((2, d, BLOCK), BF16),
            vmem((2, d, BLOCK), BF16),
            vmem((2, BLOCK, d), BF16),
            vmem((SLOTS, 2, high, cols), BF16),
            vmem((SLOTS, 2, 2, n1, cols), BF16),
            vmem((SLOTS, 2, 2, 2, n1, cols), BF16),
            vmem((2, 2, 2, n1, cols), F32),
            vmem((SLOTS, 2, 2, n2, cols), BF16),
            vmem((SLOTS, 2, 2, n2, cols), BF16),
            vmem((SLOTS, 2, 2, 2, n2, cols), BF16),
            vmem((SLOTS, 2, 2, 2, n2, cols), BF16),
            vmem((SLOTS, 2, 2, n2, cols), BF16),
            pltpu.SemaphoreType.DMA((SLOTS, STAGES, 2, 2)),
            pltpu.SemaphoreType.DMA((SLOTS, STAGES, 2, 2)),
            pltpu.SemaphoreType.DMA((2, 3)),
            pltpu.SemaphoreType.DMA((2,)),
            pltpu.SemaphoreType.DMA((SLOTS, 2)),
        ],
        compiler_params=pltpu.CompilerParams(collective_id=0, has_side_effects=True, vmem_limit_bytes=VMEM_LIMIT),
        cost_estimate=pl.CostEstimate(flops=flops, bytes_accessed=4 * wg.size * 3, transcendentals=tokens * ff * 6),
        name="train",
    )(x, dy, wg, wu, wd)


def update(d, grad_of, ins, outs):
    for i in range(3):
        for h in range(2):
            g = grad_of(i, h)
            span = slice(h * g.shape[1], (h + 1) * g.shape[1])
            where = (0, span) if i == 2 else (0, slice(None), span)
            g = (g.T if i == 2 else g).astype(F32)
            m = 0.9 * ins[3 + i][where] + 0.1 * g
            v = 0.95 * ins[6 + i][where] + 0.05 * g * g
            w = ins[i][where].astype(F32)
            step = m * lax.rsqrt(v + 1e-8) + 0.1 * w
            outs[i][where] = (w - 0.02 * step).astype(BF16)
            outs[3 + i][where] = m
            outs[6 + i][where] = v


def early_kernel(d, g_ref, *refs):
    update(d, lambda i, h: g_ref[0, h, i * d : (i + 1) * d, :], refs[:9], refs[-9:])


def late_kernel(d, side, *refs):
    pieces, ins, outs, g = (refs[:4], refs[4:8]), refs[8:17], refs[-10:-1], refs[-1]
    me = lax.axis_index("dp")
    n1 = pieces[0][0].shape[2]
    for flow, i in enumerate((me // side, lax.rem(me, side))):
        mine, left, right, far = pieces[flow]
        for by, piece in enumerate((mine, right, far, left)):
            where = pl.ds(pl.multiple_of((flow * side + lax.rem(i + by, side)) * n1, 16), n1)
            for h in range(2):
                g[h, where, :] = piece[h, 0]
    update(d, lambda i, h: g[h, i * d : (i + 1) * d, :], ins, outs)


def adamw(kernel, name, pieces, piece_specs, arrays, old, after, start, count, scratch=()):
    layers, d, ff = arrays[0].shape
    blocks = ff // BLOCK
    size = count * 3 * d * BLOCK

    def across(c):
        return layers - 1 - (c + start) // blocks, 0, lax.rem(c + start, blocks)

    def down(c):
        return layers - 1 - (c + start) // blocks, lax.rem(c + start, blocks), 0

    specs = [pl.BlockSpec((1, d, BLOCK), across), pl.BlockSpec((1, d, BLOCK), across), pl.BlockSpec((1, BLOCK, d), down)] * 3
    passed = [pl.BlockSpec(memory_space=pl.ANY)] * (len(old) + len(after))
    first = len(pieces) + len(arrays)
    return pl.pallas_call(
        kernel,
        grid=(count,),
        out_shape=[jax.ShapeDtypeStruct(one.shape, one.dtype) for one in arrays],
        in_specs=[*piece_specs, *specs, *passed],
        out_specs=specs,
        scratch_shapes=scratch,
        input_output_aliases={first + i: i for i in range(len(old))},
        compiler_params=pltpu.CompilerParams(vmem_limit_bytes=60_000_000),
        cost_estimate=pl.CostEstimate(flops=400 * size, bytes_accessed=22 * size, transcendentals=size),
        name=name,
    )(*pieces, *arrays, *old, *after)


def solution(mesh):
    side = math.isqrt(mesh.shape["dp"])
    assert side == 4 and side * side == mesh.shape["dp"]

    def ring(along_x, by):
        devices = [(i // side, i % side) for i in range(side * side)]
        return [(n, (i + by) % side * side + k if along_x else i * side + (k + by) % side) for n, (i, k) in enumerate(devices)]

    def step(x, dy, *arrays):
        d = x.shape[2]
        early, *late = gradients(side, x, dy, *arrays[:3])
        cut, _, high, cols = early.shape
        n1 = late[0].shape[2]
        left = [lax.ppermute(late[flow], "dp", ring(flow == 0, 1)) for flow in range(2)]
        right = [lax.ppermute(late[flow], "dp", ring(flow == 0, -1)) for flow in range(2)]
        middle = (cut + 1) // 2

        def early_step(name, old, after, start, stop):
            spec = pl.BlockSpec((1, 2, high, cols), lambda c: (c + start, 0, 0, 0))
            return adamw(functools.partial(early_kernel, d), name, [early], [spec], arrays, old, after, start, stop - start)

        new = early_step("adamw_first", (), (), 0, middle)
        left, right, new = lax.optimization_barrier((left, right, tuple(new)))
        far = [lax.ppermute(left[flow], "dp", ring(flow == 0, 1)) for flow in range(2)]
        new = early_step("adamw_second", new, (*left, *right), middle, cut)
        both = pl.BlockSpec((2, 1, n1, cols), lambda c: (0, c, 0, 0))
        pieces = [one for flow in range(2) for one in (late[flow], left[flow], right[flow], far[flow])]
        kernel = functools.partial(late_kernel, d, side)
        scratch = [pltpu.VMEM((2, high, cols), BF16)]
        new = adamw(kernel, "adamw_late", pieces, [both] * 8, arrays, new, (), cut, LATE, scratch)
        return tuple(new)

    return jax.shard_map(
        step,
        mesh=mesh,
        in_specs=(P(("rep", "dp"), None, None),) * 2 + (P(None, None, None),) * 9,
        out_specs=(P("rep", None, None),) * 9,
        check_vma=False,
    )
```

```python
import functools
import math

import jax
import jax.numpy as jnp
from jax import lax
from jax.experimental import pallas as pl
from jax.experimental.pallas import tpu as pltpu
from jax.sharding import PartitionSpec as P

BLOCK = 512
TILE = 1024
LATE = 4
SLOTS = 4
STAGES = 8
VMEM_LIMIT = 67_043_328
F32, BF16 = jnp.float32, jnp.bfloat16
NN = (((1,), (0,)), ((), ()))
NT = (((1,), (1,)), ((), ()))


def dot(a, b, dims=NN):
    return lax.dot_general(a, b, dims, preferred_element_type=F32)


def scale_of(wide):
    return lax.rsqrt(jnp.mean(wide * wide, -1, keepdims=True) + 1e-6)


def normed(h):
    wide = h.astype(F32)
    return (wide * scale_of(wide)).astype(BF16)


def train_kernel(
    side, x_hbm, dy_hbm, wg_hbm, wu_hbm, wd_hbm, out_hbm, late0, late1,
    x, a, at, dh, dht, act, dg, du, acc1, acc2, wg, wu, wd,
    grad, r1, r2, part, t1, u1, t2, u2, own, send, recv, w_sem, x_sem, own_sem,
):
    tokens, d = x.shape
    blocks = wg_hbm.shape[2] // BLOCK
    chunks = wg_hbm.shape[0] * blocks
    tiles = tokens // TILE
    pieces = min(8, blocks * tiles)
    wide = tokens // pieces
    cut = out_hbm.shape[0]
    lates = (late0, late1)
    half_rows = grad.shape[2] // 2
    n1, n2 = half_rows // side, half_rows // side // side
    cols = BLOCK // 2

    me = lax.axis_index("dp")
    ix, iy = me // side, lax.rem(me, side)

    def turn(i, by):
        return lax.rem(i + (by + side), side)

    along_x = (ix, tuple(turn(ix, s) * side + iy for s in (1, -1)))
    along_y = (iy, tuple(ix * side + turn(iy, s) for s in (1, -1)))
    flows = ((along_x, along_y), (along_y, along_x))
    step_of = (1, -1)

    barrier = pltpu.get_barrier_semaphore()
    for _, near in (along_x, along_y):
        for device in near:
            pl.semaphore_signal(barrier, inc=1, device_id={"dp": device}, device_id_type=pl.DeviceIdType.MESH)

    def rows(flow, s1, s2=None):
        if s2 is None:
            return pl.ds(pl.multiple_of(flow * half_rows + s1 * n1, 16), n1)
        return pl.ds(pl.multiple_of(flow * half_rows + s1 * n1 + s2 * n2, 16), n2)

    def gathered(c, flow, i1, i2, late, way=slice(None)):
        if late:
            return lates[flow].at[way, c - cut, pl.ds(pl.multiple_of(i2 * n2, 16), n2), :]
        return out_hbm.at[c, way, rows(flow, i1, i2), :]

    def hop(stage, c, flow, way, late):
        slot = lax.rem(c, SLOTS)
        (i1, near1), (i2, near2) = flows[flow]
        step = step_of[way]
        if stage == 0:
            src, dst, to = grad.at[slot, way, rows(flow, turn(i1, 2)), :], r1.at[slot, flow, way], near1
        elif stage == 1:
            src, dst, to = grad.at[slot, :, rows(flow, turn(i1, step)), :], r2.at[slot, flow, way], near1
        elif stage == 2:
            src, dst, to = t1.at[slot, flow, way], u1.at[slot, flow, way], near2
        elif stage == 3:
            src, dst, to = t2.at[slot, flow, way], u2.at[slot, flow, way], near2
        elif stage == 4:
            src, dst, to = own.at[slot, flow], gathered(c, flow, i1, i2, late), near2
        elif stage == 5:
            src = dst = gathered(c, flow, i1, turn(i2, -step), late, way)
            to = near2
        elif stage == 6:
            src = dst = out_hbm.at[c, :, rows(flow, i1), :]
            to = near1
        else:
            src = dst = out_hbm.at[c, way, rows(flow, turn(i1, -step)), :]
            to = near1
        return pltpu.make_async_remote_copy(
            src_ref=src,
            dst_ref=dst,
            send_sem=send.at[slot, stage, flow, way],
            recv_sem=recv.at[slot, stage, flow, way],
            device_id={"dp": to[way]},
            device_id_type=pl.DeviceIdType.MESH,
        )

    def keep(c, flow, late):
        slot = lax.rem(c, SLOTS)
        (i1, _), (i2, _) = flows[flow]
        return pltpu.make_async_copy(own.at[slot, flow], gathered(c, flow, i1, i2, late), own_sem.at[slot, flow])

    def wait(stage, c, late=False):
        for flow in range(2):
            for way in range(2):
                hop(stage, c, flow, way, late).wait()

    def start(stage, c, late=False, flows=(0, 1)):
        for flow in flows:
            for way in range(2):
                hop(stage, c, flow, way, late).start()

    def advance(event, c, late):
        slot, pslot = lax.rem(c, SLOTS), lax.rem(c, 2)
        wait(event - 1, c, late)
        for flow in range(2):
            (i1, _), (i2, _) = flows[flow]
            if event == 1:
                for way in range(2):
                    where = rows(flow, turn(i1, step_of[way]))
                    total = grad[slot, way, where, :].astype(F32) + r1[slot, flow, way].astype(F32)
                    grad[slot, way, where, :] = total.astype(BF16)
            elif event == 2:
                for h in range(2):
                    mine = grad[slot, h, rows(flow, i1), :].astype(F32)
                    part[pslot, flow, h] = mine + r2[slot, flow, 0, h].astype(F32) + r2[slot, flow, 1, h].astype(F32)
                far = pl.ds(pl.multiple_of(turn(i2, 2) * n2, 16), n2)
                for way in range(2):
                    t1[slot, flow, way] = part[pslot, flow, way, far, :].astype(BF16)
            elif event == 3:
                for way in range(2):
                    near = pl.ds(pl.multiple_of(turn(i2, step_of[way]) * n2, 16), n2)
                    for h in range(2):
                        total = part[pslot, flow, h, near, :]
                        if h == way:
                            total = total + u1[slot, flow, way].astype(F32)
                        t2[slot, flow, way, h] = total.astype(BF16)
            elif event == 4:
                here = pl.ds(pl.multiple_of(i2 * n2, 16), n2)
                for h in range(2):
                    total = part[pslot, flow, h, here, :] + u2[slot, flow, 0, h].astype(F32) + u2[slot, flow, 1, h].astype(F32)
                    own[slot, flow, h] = total.astype(BF16)
                keep(c, flow, late).start()
            elif event == 5:
                keep(c, flow, late).wait()
        if event < (6 if late else STAGES):
            start(event, c, late)

    def poll(k, events):
        for behind, event in events:
            c = k - behind

            @pl.when((c >= 0) & (c < (cut if event > 3 else chunks)))
            def _(c=c, event=event):
                advance(event, c, False)

            if 3 < event < 7:

                @pl.when((c >= cut) & (c < chunks))
                def _(c=c, event=event):
                    advance(event, c, True)

    def poll_mid(k):
        poll(k, ((4, 7), (3, 5), (2, 3)))

    def poll_first(k):
        poll(k, ((1, 1),))

    def poll_end(k):
        poll(k, ((4, 8), (3, 6), (2, 4), (1, 2)))

    def weights(b):
        layer, j, slot = lax.rem(b // blocks, 2), lax.rem(b, blocks), lax.rem(b, 2)
        span = pl.ds(pl.multiple_of(j * BLOCK, BLOCK), BLOCK)
        return (
            pltpu.make_async_copy(wg_hbm.at[layer, :, span], wg.at[slot], w_sem.at[slot, 0]),
            pltpu.make_async_copy(wu_hbm.at[layer, :, span], wu.at[slot], w_sem.at[slot, 1]),
            pltpu.make_async_copy(wd_hbm.at[layer, span, :], wd.at[slot], w_sem.at[slot, 2]),
        )

    def next_weights(b):
        for copy in weights(b):
            copy.wait()

        @pl.when(b + 1 < 3 * blocks)
        def _():
            for copy in weights(b + 1):
                copy.start()

    def each_tile(body):
        @pl.loop(0, tiles)
        def _(t):
            body(pl.ds(pl.multiple_of(t * TILE, TILE), TILE))

    load_x = pltpu.make_async_copy(x_hbm.at[0], x, x_sem.at[0])
    load_dy = pltpu.make_async_copy(dy_hbm.at[0], dh, x_sem.at[1])
    load_x.start()
    for copy in weights(0):
        copy.start()
    load_dy.start()
    load_x.wait()

    def first(t):
        a[t, :] = normed(x[t, :])
        acc1[t, :] = jnp.zeros((TILE, d), F32)

    each_tile(first)

    @pl.loop(0, blocks)
    def _(b):
        next_weights(b)
        slot = lax.rem(b, 2)

        @pl.when(b == 0)
        def _():
            load_dy.wait()

        def forward(t, n):
            gate = dot(a[t, :], wg[slot])
            up = dot(a[t, :], wu[slot])
            acc1[t, :] += dot((jax.nn.silu(gate) * up).astype(BF16), wd[slot])

            piece = pl.ds(pl.multiple_of(lax.rem(b * tiles + n, pieces) * wide, wide), wide)
            dht[:, piece] = dh[piece, :].T

        @pl.loop(0, tiles)
        def _(n):
            forward(pl.ds(pl.multiple_of(n * TILE, TILE), TILE), n)


    def second(t):
        h = (x[t, :].astype(F32) + acc1[t, :].astype(BF16).astype(F32)).astype(BF16)
        x[t, :] = h
        after = normed(h)
        a[t, :] = after
        at[:, t] = after.T
        acc1[t, :] = jnp.zeros((TILE, d), F32)
        acc2[t, :] = jnp.zeros((TILE, d), F32)

    each_tile(second)
    pl.semaphore_wait(barrier, 4)

    def backward(k, to_input):
        next_weights(k + blocks)
        slot, gslot = lax.rem(k + blocks, 2), lax.rem(k, SLOTS)

        def states(t):
            gate = dot(a[t, :], wg[slot])
            up = dot(a[t, :], wu[slot])
            by_act = dot(dh[t, :], wd[slot], NT).astype(BF16).astype(F32)
            s = jax.nn.sigmoid(gate)
            silu = gate * s
            act[t, :] = (silu * up).astype(BF16)
            by_up = (by_act * silu).astype(BF16)
            by_gate = (by_act * up * (s * (1.0 + gate * (1.0 - s)))).astype(BF16)
            dg[t, :] = by_gate
            du[t, :] = by_up
            if to_input:
                acc1[t, :] += dot(by_gate, wg[slot], NT)
                acc2[t, :] += dot(by_up, wu[slot], NT)

        @pl.loop(0, tiles)
        def _(t):
            states(pl.ds(pl.multiple_of(t * TILE, TILE), TILE))

            @pl.when(t == 0)
            def _():
                poll_first(k)

        poll_mid(k)
        spans = [slice(h * cols, (h + 1) * cols) for h in range(2)]
        for h, span in enumerate(spans):
            grad[gslot, h, 0:d, :] = dot(at[...], dg[:, span]).astype(BF16)
            grad[gslot, h, d : 2 * d, :] = dot(at[...], du[:, span]).astype(BF16)
        start(0, k, flows=(0,))
        for h, span in enumerate(spans):
            grad[gslot, h, 2 * d : 3 * d, :] = dot(dht[...], act[:, span]).astype(BF16)
        start(0, k, flows=(1,))
        poll_end(k)

    @pl.loop(0, blocks)
    def _(k):
        backward(k, True)

    def between(t):
        by_a = (acc1[t, :].astype(BF16).astype(F32) + acc2[t, :].astype(BF16).astype(F32)).astype(BF16).astype(F32)
        wide = x[t, :].astype(F32)
        scale = scale_of(wide)
        along = jnp.sum(by_a * wide, -1, keepdims=True) * (scale * scale * scale / d)
        by_h = (by_a * scale - wide * along).astype(BF16)
        total = (dh[t, :].astype(F32) + by_h.astype(F32)).astype(BF16)
        dh[t, :] = total
        dht[:, t] = total.T

    each_tile(between)
    load_x.start()
    load_x.wait()

    def first_again(t):
        before = normed(x[t, :])
        a[t, :] = before
        at[:, t] = before.T

    each_tile(first_again)

    @pl.loop(blocks, 2 * blocks)
    def _(k):
        backward(k, False)

    @pl.loop(2 * blocks, 2 * blocks + 3)
    def _(k):
        poll_first(k)
        poll_mid(k)
        poll_end(k)


def gradients(side, x, dy, wg, wu, wd):
    _, tokens, d = x.shape
    layers, _, ff = wg.shape
    chunks, high, cols = layers * ff // BLOCK, 3 * d, BLOCK // 2
    n1, n2 = high // 2 // side, high // 2 // side // side
    flops = 2 * tokens * d * ff * 17
    vmem = pltpu.VMEM
    return pl.pallas_call(
        functools.partial(train_kernel, side),
        out_shape=[
            jax.ShapeDtypeStruct((chunks - LATE, 2, high, cols), BF16),
            jax.ShapeDtypeStruct((2, LATE, n1, cols), BF16),
            jax.ShapeDtypeStruct((2, LATE, n1, cols), BF16),
        ],
        in_specs=[pl.BlockSpec(memory_space=pl.ANY)] * 5,
        out_specs=[pl.BlockSpec(memory_space=pl.ANY)] * 3,
        scratch_shapes=[
            vmem((tokens, d), BF16),
            vmem((tokens, d), BF16),
            vmem((d, tokens), BF16),
            vmem((tokens, d), BF16),
            vmem((d, tokens), BF16),
            vmem((tokens, BLOCK), BF16),
            vmem((tokens, BLOCK), BF16),
            vmem((tokens, BLOCK), BF16),
            vmem((tokens, d), F32),
            vmem((tokens, d), F32),
            vmem((2, d, BLOCK), BF16),
            vmem((2, d, BLOCK), BF16),
            vmem((2, BLOCK, d), BF16),
            vmem((SLOTS, 2, high, cols), BF16),
            vmem((SLOTS, 2, 2, n1, cols), BF16),
            vmem((SLOTS, 2, 2, 2, n1, cols), BF16),
            vmem((2, 2, 2, n1, cols), F32),
            vmem((SLOTS, 2, 2, n2, cols), BF16),
            vmem((SLOTS, 2, 2, n2, cols), BF16),
            vmem((SLOTS, 2, 2, 2, n2, cols), BF16),
            vmem((SLOTS, 2, 2, 2, n2, cols), BF16),
            vmem((SLOTS, 2, 2, n2, cols), BF16),
            pltpu.SemaphoreType.DMA((SLOTS, STAGES, 2, 2)),
            pltpu.SemaphoreType.DMA((SLOTS, STAGES, 2, 2)),
            pltpu.SemaphoreType.DMA((2, 3)),
            pltpu.SemaphoreType.DMA((2,)),
            pltpu.SemaphoreType.DMA((SLOTS, 2)),
        ],
        compiler_params=pltpu.CompilerParams(collective_id=0, has_side_effects=True, vmem_limit_bytes=VMEM_LIMIT),
        cost_estimate=pl.CostEstimate(flops=flops, bytes_accessed=4 * wg.size * 3, transcendentals=tokens * ff * 6),
        name="train",
    )(x, dy, wg, wu, wd)


def update(d, grad_of, ins, outs):
    for i in range(3):
        for h in range(2):
            g = grad_of(i, h)
            span = slice(h * g.shape[1], (h + 1) * g.shape[1])
            where = (0, span) if i == 2 else (0, slice(None), span)
            g = (g.T if i == 2 else g).astype(F32)
            m = 0.9 * ins[3 + i][where] + 0.1 * g
            v = 0.95 * ins[6 + i][where] + 0.05 * g * g
            w = ins[i][where].astype(F32)
            step = m * lax.rsqrt(v + 1e-8) + 0.1 * w
            outs[i][where] = (w - 0.02 * step).astype(BF16)
            outs[3 + i][where] = m
            outs[6 + i][where] = v


def early_kernel(d, g_ref, *refs):
    update(d, lambda i, h: g_ref[0, h, i * d : (i + 1) * d, :], refs[:9], refs[-9:])


def late_kernel(d, side, *refs):
    pieces, ins, outs, g = (refs[:4], refs[4:8]), refs[8:17], refs[-10:-1], refs[-1]
    me = lax.axis_index("dp")
    n1 = pieces[0][0].shape[2]
    for flow, i in enumerate((me // side, lax.rem(me, side))):
        mine, left, right, far = pieces[flow]
        for by, piece in enumerate((mine, right, far, left)):
            where = pl.ds(pl.multiple_of((flow * side + lax.rem(i + by, side)) * n1, 16), n1)
            for h in range(2):
                g[h, where, :] = piece[h, 0]
    update(d, lambda i, h: g[h, i * d : (i + 1) * d, :], ins, outs)


def adamw(kernel, name, pieces, piece_specs, arrays, old, after, start, count, scratch=()):
    layers, d, ff = arrays[0].shape
    blocks = ff // BLOCK
    size = count * 3 * d * BLOCK

    def across(c):
        return layers - 1 - (c + start) // blocks, 0, lax.rem(c + start, blocks)

    def down(c):
        return layers - 1 - (c + start) // blocks, lax.rem(c + start, blocks), 0

    specs = [pl.BlockSpec((1, d, BLOCK), across), pl.BlockSpec((1, d, BLOCK), across), pl.BlockSpec((1, BLOCK, d), down)] * 3
    passed = [pl.BlockSpec(memory_space=pl.ANY)] * (len(old) + len(after))
    first = len(pieces) + len(arrays)
    return pl.pallas_call(
        kernel,
        grid=(count,),
        out_shape=[jax.ShapeDtypeStruct(one.shape, one.dtype) for one in arrays],
        in_specs=[*piece_specs, *specs, *passed],
        out_specs=specs,
        scratch_shapes=scratch,
        input_output_aliases={first + i: i for i in range(len(old))},
        compiler_params=pltpu.CompilerParams(vmem_limit_bytes=60_000_000),
        cost_estimate=pl.CostEstimate(flops=400 * size, bytes_accessed=22 * size, transcendentals=size),
        name=name,
    )(*pieces, *arrays, *old, *after)


def solution(mesh):
    side = math.isqrt(mesh.shape["dp"])
    assert side == 4 and side * side == mesh.shape["dp"]

    def ring(along_x, by):
        devices = [(i // side, i % side) for i in range(side * side)]
        return [(n, (i + by) % side * side + k if along_x else i * side + (k + by) % side) for n, (i, k) in enumerate(devices)]

    def step(x, dy, *arrays):
        d = x.shape[2]
        early, *late = gradients(side, x, dy, *arrays[:3])
        cut, _, high, cols = early.shape
        n1 = late[0].shape[2]
        left = [lax.ppermute(late[flow], "dp", ring(flow == 0, 1)) for flow in range(2)]
        right = [lax.ppermute(late[flow], "dp", ring(flow == 0, -1)) for flow in range(2)]
        middle = (cut + 1) // 2

        def early_step(name, old, after, start, stop):
            spec = pl.BlockSpec((1, 2, high, cols), lambda c: (c + start, 0, 0, 0))
            return adamw(functools.partial(early_kernel, d), name, [early], [spec], arrays, old, after, start, stop - start)

        new = early_step("adamw_first", (), (), 0, middle)
        left, right, new = lax.optimization_barrier((left, right, tuple(new)))
        far = [lax.ppermute(left[flow], "dp", ring(flow == 0, 1)) for flow in range(2)]
        new = early_step("adamw_second", new, (*left, *right), middle, cut)
        both = pl.BlockSpec((2, 1, n1, cols), lambda c: (0, c, 0, 0))
        pieces = [one for flow in range(2) for one in (late[flow], left[flow], right[flow], far[flow])]
        kernel = functools.partial(late_kernel, d, side)
        scratch = [pltpu.VMEM((2, high, cols), BF16)]
        new = adamw(kernel, "adamw_late", pieces, [both] * 8, arrays, new, (), cut, LATE, scratch)
        return tuple(new)

    return jax.shard_map(
        step,
        mesh=mesh,
        in_specs=(P(("rep", "dp"), None, None),) * 2 + (P(None, None, None),) * 9,
        out_specs=(P("rep", None, None),) * 9,
        check_vma=False,
    )
```
